128 devices in a mesh: seq: 128 (over z, y, x, core).
Axes of the slice: x: 4, y: 4, z: 4, core: 2. Of those that a mesh axis runs over, the one named last changes fastest.
Arguments:
- queries: bfloat16 [2, 4, 128, 576], replicated, may hold values from -40 to 40
- latent_cache: bfloat16 [2, 524288, 576], P(None, 'seq'), may hold values from -6 to 6
- lengths: int32 [2], replicated, may hold values from 65536 to 524288
- offsets: int32 [2, 4], replicated, may hold values from 0 to 3
Outputs:
- attended: bfloat16 [2, 4, 128, 512], replicated
The draws below stay inside these ranges and needn't reach their ends.
All inputs are finite; a program needn't handle non-finite values.
Results may differ from the reference program's by a relative error of at most 0.001.
The reference program's roundings to bfloat16 on the way count: a program that leaves them out, or rounds other values in their place, can miss the bound.
Values may be sent and summed in bfloat16 or wider, within the bound.
No kernel may reach another device: no remote copies, remote signals or barrier semaphores. Data moves between devices by JAX's collectives and lax.ppermute only.
A program may use at most 128 MiB of HBM per device.

```python
import jax
import jax.numpy as jnp
from jax import lax

HEADS = 128
LATENT = 512
ROPE = 64
QTOK = 4
REQS = 2
CACHE_DEV = 4096
SEQ = 524288
N_SEQ = 128


def special(key):
    base = jax.random.fold_in(key, 11)
    key_vec, key_noise, key_spot, key_strength = jax.random.split(base, 4)
    count = 2 * REQS
    width = LATENT + ROPE
    signs = jnp.where(jax.random.normal(key_vec, (count, width), jnp.float32) > 0.0, 2.0, -2.0)
    vectors = signs.astype(jnp.float32)
    noise = 0.5 * jax.random.normal(key_noise, (count, width), jnp.float32)
    along = jnp.sum(noise * vectors, axis=1, keepdims=True) / (4.0 * width)
    across = noise - along * vectors
    targets = 120.0 + 100.0 * jax.random.randint(key_strength, (count,), 0, 4).astype(jnp.float32)
    shrink = 1.0 - 2.0 / targets
    twins = jnp.clip(shrink[:, None] * vectors + across, -6.0, 6.0)
    strengths = targets / (4.0 * width * 192.0 ** (-0.5))
    stride = SEQ // 16
    spots = jnp.arange(count) // REQS * stride + jax.random.randint(key_spot, (count,), 0, stride - 8)
    return (vectors, twins, spots, strengths)


def draw_latent_cache(key, part):
    shape = (REQS, SEQ, LATENT + ROPE)
    cache = jax.random.normal(jax.random.fold_in(key, 3), shape, jnp.float32)
    vectors, twins, spots, strengths = special(key)
    owners = jnp.arange(2 * REQS) % REQS
    cache = cache.at[owners, spots].set(vectors)
    cache = cache.at[owners, spots + 1].set(twins)
    return jnp.clip(cache, -6.0, 6.0).astype(jnp.bfloat16)


def draw_queries(key, part):
    shape = (REQS, QTOK, HEADS, LATENT + ROPE)
    values = jnp.clip(jax.random.normal(jax.random.fold_in(key, 5), shape, jnp.float32), -6.0, 6.0)
    vectors, twins, spots, strengths = special(key)
    counter = jnp.arange(2 * REQS)
    owners = counter % REQS
    tokens = counter % QTOK
    chosen = counter * 7 % HEADS
    aligned = strengths[:, None] * vectors
    values = values.at[owners, tokens, chosen].set(jnp.clip(aligned, -40.0, 40.0))
    return values.astype(jnp.bfloat16)


def place_ends(array, rng, least, largest):
    shape = array.shape
    place = [jax.random.randint(jax.random.fold_in(rng, axis), (), 0, shape[axis]) for axis in range(len(shape))]
    array = array.at[tuple(place)].set(least)
    longest = shape.index(max(shape))
    place[longest] = (place[longest] + 1) % shape[longest]
    return array.at[tuple(place)].set(largest)


def setup_inputs(seed: int = 0) -> dict:
    splits = jax.random.split(jax.random.key(seed), 5)
    return {
        "queries": draw_queries(jax.random.fold_in(splits[4], 71), 0),
        "latent_cache": draw_latent_cache(jax.random.fold_in(splits[4], 71), 0),
        "lengths": jax.random.randint(splits[2], (REQS,), SEQ // 8, SEQ + 1).astype(jnp.int32),
        "offsets": place_ends(jax.random.randint(splits[3], (REQS, QTOK), 0, QTOK), jax.random.fold_in(splits[3], 1), 0, QTOK - 1).astype(jnp.int32),
    }


softmax_scale = 192.0 ** -0.5


def one_request(operands):
    query, cache, length, offset = operands
    rows = query.reshape(QTOK * HEADS, LATENT + ROPE)
    limit = jnp.repeat(length - QTOK + 1 + offset, HEADS)

    def block(index):
        keys = lax.dynamic_slice_in_dim(cache, (index * CACHE_DEV).astype(jnp.int32), CACHE_DEV, 0)
        score = jnp.dot(rows, keys.T, preferred_element_type=jnp.float32) * softmax_scale
        places = index * CACHE_DEV + jnp.arange(CACHE_DEV, dtype=jnp.int32)
        visible = places[None, :] < limit[:, None]
        score = jnp.where(visible, score, -1e30)
        peak = jnp.max(score, axis=1)
        weight = jnp.where(visible, jnp.exp(score - peak[:, None]), 0.0)
        total = jnp.sum(weight, axis=1)
        partial_value = jnp.dot(weight.astype(jnp.bfloat16), keys[:, :LATENT], preferred_element_type=jnp.float32)
        return peak, total, partial_value

    peaks, totals, partials = lax.map(block, jnp.arange(N_SEQ, dtype=jnp.int32))
    top = jnp.max(peaks, axis=0)
    factor = jnp.exp(peaks - top[None, :])
    upper = jnp.sum(factor[:, :, None] * partials, axis=0)
    lower = jnp.sum(factor * totals, axis=0)
    return (upper / lower[:, None]).astype(jnp.bfloat16).reshape(QTOK, HEADS, LATENT)


def reference(queries, latent_cache, lengths, offsets):
    return lax.map(one_request, (queries, latent_cache, lengths, offsets))
```

```python
import functools

import jax
import jax.numpy as jnp
from jax import lax
from jax.experimental import pallas as pl
from jax.experimental.pallas import tpu as pltpu
from jax.sharding import Mesh
from jax.sharding import PartitionSpec as P

LATENT = 512
CHIPS = ("seq_0", "seq_1", "seq_2")
CORE = "seq_3"
SEQ = (*CHIPS, CORE)
LANES = 128
HIDDEN = -1e30
SCALE = 192.0 ** (-0.5)
LOG2E = 1.4426950408889634
CHUNK = 1024
F32 = jnp.float32
VMEM_LIMIT = 60 * 1024 * 1024
whole = functools.partial(pl.BlockSpec, memory_space=pltpu.VMEM)


def block_partial(lengths, offsets, query_hbm, cache_hbm, out, stats, query, rows_q, keys, score, sems, *, own):
    qtokens, _, heads = query.shape
    rows = qtokens * heads
    positions = keys.shape[1]
    core = lax.axis_index(CORE)
    request = core if own else 1 - core
    start = lax.axis_index(SEQ) * positions

    def key_copy(j):
        part = pl.ds(j * CHUNK, CHUNK)
        return pltpu.make_async_copy(cache_hbm.at[request, :, part], keys.at[:, part], sems.at[j])

    query_copy = pltpu.make_async_copy(query_hbm.at[request], query, sems.at[positions // CHUNK])
    query_copy.start()
    for j in range(positions // CHUNK):
        key_copy(j).start()
    stats[...] = jnp.full((rows, LANES), HIDDEN, F32)
    lane = lax.broadcasted_iota(jnp.int32, (heads, CHUNK), 1)
    query_copy.wait()
    for t in range(qtokens):
        rows_q[t * heads : (t + 1) * heads, :] = query[t].T

    for j in range(positions // CHUNK):
        part = slice(j * CHUNK, (j + 1) * CHUNK)
        key_copy(j).wait()
        product = jnp.dot(rows_q[:, :LATENT], keys[:LATENT, part], preferred_element_type=F32)
        product += jnp.dot(rows_q[:, LATENT:], keys[LATENT:, part], preferred_element_type=F32)
        for t in range(qtokens):
            r = slice(t * heads, (t + 1) * heads)
            limit = lengths[request] - qtokens + 1 + offsets[request, t] - start
            seen = jnp.where(lane < limit - j * CHUNK, product[r], HIDDEN)
            score[r, part] = seen
            top = stats[r, :]
            for u in range(CHUNK // LANES):
                top = jnp.maximum(top, seen[:, u * LANES : (u + 1) * LANES])
            stats[r, :] = top

    peak = jnp.max(stats[...], axis=1, keepdims=True)
    base = jnp.where(peak < 0.1 * HIDDEN, 0.0, peak)
    total = jnp.zeros((rows, LANES), F32)
    for j in range(positions // CHUNK):
        part = slice(j * CHUNK, (j + 1) * CHUNK)
        weight = jnp.exp2((score[:, part] - base) * (SCALE * LOG2E))
        for u in range(CHUNK // LANES):
            total = total + weight[:, u * LANES : (u + 1) * LANES]
        value = lax.dot_general(
            weight.astype(jnp.bfloat16),
            keys[:LATENT, part],
            (((1,), (1,)), ((), ())),
            preferred_element_type=F32,
        )
        if j == 0:
            out[...] = value
        else:
            out[...] += value
    total = jnp.sum(total, axis=1, keepdims=True)
    left = lax.broadcasted_iota(jnp.int32, (rows, LANES), 1) < LANES // 2
    stats[...] = jnp.where(left, peak, total)


def partials(lengths, offsets, query, cache, own):
    _, qtokens, width, heads = query.shape
    positions = cache.shape[2]
    rows = qtokens * heads
    scalars = pl.BlockSpec(memory_space=pltpu.SMEM)
    arrays = pl.BlockSpec(memory_space=pl.ANY)
    return pl.pallas_call(
        functools.partial(block_partial, own=own),
        in_specs=[scalars, scalars, arrays, arrays],
        out_specs=[whole(), whole()],
        out_shape=[
            jax.ShapeDtypeStruct((rows, LATENT), F32),
            jax.ShapeDtypeStruct((rows, LANES), F32),
        ],
        scratch_shapes=[
            pltpu.VMEM((qtokens, width, heads), jnp.bfloat16),
            pltpu.VMEM((rows, width), jnp.bfloat16),
            pltpu.VMEM((width, positions), jnp.bfloat16),
            pltpu.VMEM((rows, positions), F32),
            pltpu.SemaphoreType.DMA((positions // CHUNK + 1,)),
        ],
        compiler_params=pltpu.CompilerParams(vmem_limit_bytes=VMEM_LIMIT),
        cost_estimate=pl.CostEstimate(
            flops=2 * rows * positions * (width + LATENT),
            bytes_accessed=2 * positions * width,
            transcendentals=rows * positions,
        ),
        name="block_partial",
    )(lengths, offsets, query, cache)


def merge(out_a, stats_a, out_b, stats_b, packed):
    peak_a, total_a = stats_a[:, :1], stats_a[:, LANES // 2 : LANES // 2 + 1]
    peak_b, total_b = stats_b[:, :1], stats_b[:, LANES // 2 : LANES // 2 + 1]
    peak = jnp.maximum(peak_a, peak_b)
    factor_a = jnp.exp2((peak_a - peak) * (SCALE * LOG2E))
    factor_b = jnp.exp2((peak_b - peak) * (SCALE * LOG2E))
    packed[:, :LATENT] = factor_a * out_a[...] + factor_b * out_b[...]
    total = factor_a * total_a + factor_b * total_b
    left = lax.broadcasted_iota(jnp.int32, stats_a.shape, 1) < LANES // 2
    packed[:, LATENT:] = jnp.where(left, peak, total)


def finish(packed, copies):
    chips = packed.shape[0]
    stats = packed[:, :, LATENT:]
    peaks, totals = stats[:, :, :1], stats[:, :, LANES // 2 : LANES // 2 + 1]
    factor = jnp.exp2((peaks - jnp.max(peaks, axis=0, keepdims=True)) * (SCALE * LOG2E))
    lower = jnp.sum(factor * totals, axis=0)
    upper = jnp.sum(factor * packed[:, :, :LATENT], axis=0)
    rows = (upper / lower).astype(jnp.bfloat16)
    copies[...] = jnp.broadcast_to(rows[None], (chips, *rows.shape))


def on_device(queries, latent_cache, lengths, offsets):
    requests, qtokens, heads, width = queries.shape
    rows = qtokens * heads
    chips = lax.axis_size(CHIPS)
    query = jnp.transpose(queries, (0, 1, 3, 2))
    cache = jnp.transpose(latent_cache, (0, 2, 1))
    swap = [(0, 1), (1, 0)]

    lent = partials(lengths, offsets, query, cache, False)
    lent = [lax.ppermute(a, CORE, swap) for a in lent]
    kept = partials(lengths, offsets, query, cache, True)
    packed = pl.pallas_call(
        merge,
        in_specs=[whole()] * 4,
        out_specs=whole(),
        out_shape=jax.ShapeDtypeStruct((rows, LATENT + LANES), F32),
        name="merge",
    )(*kept, *lent)
    packed = packed.reshape(chips, rows // chips, LATENT + LANES)
    packed = lax.all_to_all(packed, CHIPS, 0, 0, tiled=True)
    copies = pl.pallas_call(
        finish,
        in_specs=[whole()],
        out_specs=whole(),
        out_shape=jax.ShapeDtypeStruct((chips, rows // chips, LATENT), jnp.bfloat16),
        name="finish",
    )(packed)
    mine = lax.all_to_all(copies, CHIPS, 0, 0, tiled=True).reshape(rows, LATENT)
    other = lax.ppermute(mine, CORE, swap)
    first = lax.axis_index(CORE) == 0
    both = jnp.where(first, jnp.stack([mine, other]), jnp.stack([other, mine]))
    return both.reshape(requests, qtokens, heads, LATENT)


def solution(mesh):
    torus = Mesh(mesh.devices.reshape(4, 4, 4, 2), SEQ)
    in_specs = (P(), P(None, SEQ, None), P(), P())
    return jax.shard_map(
        on_device, mesh=torus, in_specs=in_specs, out_specs=P(), check_vma=False
    )
```

```python
import functools

import jax
import jax.numpy as jnp
from jax import lax
from jax.experimental import pallas as pl
from jax.experimental.pallas import tpu as pltpu
from jax.sharding import Mesh
from jax.sharding import PartitionSpec as P

LATENT = 512
CHIPS = ("seq_0", "seq_1", "seq_2")
CORE = "seq_3"
SEQ = (*CHIPS, CORE)
LANES = 128
HIDDEN = -1e30
LOG2_SCALE = 192.0 ** (-0.5) * 1.4426950408889634
CHUNK = 1024
STEPS = 32000.0
FINE = 32768.0
F32 = jnp.float32
whole = functools.partial(pl.BlockSpec, memory_space=pltpu.VMEM)
anywhere = functools.partial(pl.BlockSpec, memory_space=pltpu.HBM)


def attend(request, limits, rows_q, keys, score, triple, ready):
    lengths, offsets = limits
    rows, positions = score.shape
    qtokens = offsets.shape[1]
    heads = rows // qtokens
    start = lax.axis_index(SEQ) * positions
    lane = lax.broadcasted_iota(jnp.int32, (heads, CHUNK), 1)
    stats = triple.at[:, LATENT:]
    stats[...] = jnp.full((rows, LANES), HIDDEN, F32)
    for j in range(positions // CHUNK):
        part = slice(j * CHUNK, (j + 1) * CHUNK)
        ready(j)
        product = jnp.dot(rows_q[:, :LATENT], keys[:LATENT, part], preferred_element_type=F32)
        product += jnp.dot(rows_q[:, LATENT:], keys[LATENT:, part], preferred_element_type=F32)
        for t in range(qtokens):
            r = slice(t * heads, (t + 1) * heads)
            limit = lengths[request] - qtokens + 1 + offsets[request, t] - start
            seen = jnp.where(lane < limit - j * CHUNK, product[r], HIDDEN)
            score[r, part] = seen
            top = stats[r, :]
            for u in range(CHUNK // LANES):
                top = jnp.maximum(top, seen[:, u * LANES : (u + 1) * LANES])
            stats[r, :] = top

    peak = jnp.max(stats[...], axis=1, keepdims=True)
    base = jnp.where(peak < 0.1 * HIDDEN, 0.0, peak)
    total = jnp.zeros((rows, LANES), F32)
    for j in range(positions // CHUNK):
        part = slice(j * CHUNK, (j + 1) * CHUNK)
        weight = jnp.exp2((score[:, part] - base) * LOG2_SCALE)
        for u in range(CHUNK // LANES):
            total = total + weight[:, u * LANES : (u + 1) * LANES]
        value = lax.dot_general(
            weight.astype(jnp.bfloat16),
            keys[:LATENT, part],
            (((1,), (1,)), ((), ())),
            preferred_element_type=F32,
        )
        if j == 0:
            triple[:, :LATENT] = value
        else:
            triple[:, :LATENT] += value
    total = jnp.sum(total, axis=1, keepdims=True)
    left = lax.broadcasted_iota(jnp.int32, (rows, LANES), 1) < LANES // 2
    stats[...] = jnp.where(left, peak, total)


def scalar_copies(arrays, refs, sems):
    return [pltpu.make_async_copy(a, r, sems.at[i]) for i, (a, r) in enumerate(zip(arrays, refs))]


def lend(lengths, offsets, queries, cache, triple, next_q, next_keys, query, rows_q, keys, score, lens, offs, sems, key_sems, next_sems):
    positions = keys.shape[1]
    qtokens, _, heads = query.shape[1:]
    core = lax.axis_index(CORE)
    scalars = scalar_copies((lengths, offsets), (lens, offs), sems)
    query_copy = pltpu.make_async_copy(queries, query, sems.at[2])

    def key_copy(request, into, own_sems, j):
        part = pl.ds(j * CHUNK, CHUNK)
        return pltpu.make_async_copy(cache.at[request, :, part], into.at[:, part], own_sems.at[j])

    parts = range(positions // CHUNK)
    first = [key_copy(1 - core, keys, key_sems, j) for j in parts]
    later = [key_copy(core, next_keys, next_sems, j) for j in parts]
    query_copy.start()
    for copy in (*scalars, *first, *later):
        copy.start()
    query_copy.wait()
    for t in range(qtokens):
        rows_q[t * heads : (t + 1) * heads, :] = query[1 - core, t].T
        next_q[t * heads : (t + 1) * heads, :] = query[core, t].T
    for copy in scalars:
        copy.wait()
    attend(1 - core, (lens, offs), rows_q, keys, score, triple, lambda j: first[j].wait())
    for copy in later:
        copy.wait()


def keep(lengths, offsets, rows_q, keys, triple, score, lens, offs, sems):
    scalars = scalar_copies((lengths, offsets), (lens, offs), sems)
    for copy in scalars:
        copy.start()
    for copy in scalars:
        copy.wait()
    attend(lax.axis_index(CORE), (lens, offs), rows_q, keys, score, triple, lambda j: None)


def in_parts(x):
    whole_part = jnp.round(x)
    rest = (x - whole_part) * FINE
    middle = jnp.round(rest)
    return [whole_part, middle, jnp.round((rest - middle) * FINE)]


def from_parts(stats, at):
    a, b, c = (stats[..., at + i : at + i + 1] for i in range(3))
    return a + (b + c * (1.0 / FINE)) * (1.0 / FINE)


def merge(kept, lent, packed):
    half = LATENT + LANES // 2
    peak_a, peak_b = kept[:, LATENT : LATENT + 1], lent[:, LATENT : LATENT + 1]
    peak = jnp.maximum(peak_a, peak_b)
    factor_a = jnp.exp2((peak_a - peak) * LOG2_SCALE)
    factor_b = jnp.exp2((peak_b - peak) * LOG2_SCALE)
    total = factor_a * kept[:, half : half + 1] + factor_b * lent[:, half : half + 1]
    values = factor_a * kept[:, :LATENT] + factor_b * lent[:, :LATENT]
    largest = jnp.max(jnp.abs(values), axis=1, keepdims=True)
    largest = jnp.where(largest > 0.0, largest, 1.0)
    packed[:, :LATENT] = jnp.round(values * (STEPS / largest)).astype(jnp.int32).astype(jnp.int16)
    level = jnp.maximum(peak * LOG2_SCALE, -STEPS)
    numbers = [*in_parts(level), *in_parts(total), *in_parts(jnp.log2(largest))]
    lane = lax.broadcasted_iota(jnp.int32, (kept.shape[0], LANES), 1)
    stats = jnp.zeros(lane.shape, F32)
    for i, number in enumerate(numbers):
        stats = jnp.where(lane == i, number, stats)
    packed[:, LATENT:] = stats.astype(jnp.int32).astype(jnp.int16)


def finish(packed, copies):
    chips, rows, _ = packed.shape
    stats = packed[:, :, LATENT:].astype(jnp.int32).astype(F32)
    level = from_parts(stats, 0)
    level = level - jnp.max(level, axis=0, keepdims=True)
    lower = jnp.sum(jnp.exp2(level) * from_parts(stats, 3), axis=0)
    factor = jnp.exp2(level + from_parts(stats, 6)) * (1.0 / STEPS)
    values = packed[:, :, :LATENT].astype(jnp.int32).astype(F32)
    upper = jnp.sum(factor * values, axis=0)
    final = (upper / lower).astype(jnp.bfloat16)
    copies[...] = jnp.broadcast_to(final[None], copies.shape)


def on_device(queries, latent_cache, lengths, offsets):
    requests, qtokens, heads, width = queries.shape
    positions = latent_cache.shape[1]
    rows = qtokens * heads
    chips = lax.axis_size(CHIPS)
    in_hbm = lambda a: pltpu.with_memory_space_constraint(a, pltpu.HBM)
    query = in_hbm(jnp.transpose(queries, (0, 1, 3, 2)))
    cache = in_hbm(jnp.transpose(latent_cache, (0, 2, 1)))
    lengths, offsets = in_hbm(lengths), in_hbm(offsets)
    swap = [(0, 1), (1, 0)]
    parts = positions // CHUNK
    limits = [pltpu.SMEM(lengths.shape, jnp.int32), pltpu.SMEM(offsets.shape, jnp.int32)]
    score = pltpu.VMEM((rows, positions), F32)
    triple = pltpu.VMEM((rows, LATENT + LANES), F32)
    cost = pl.CostEstimate(
        flops=2 * rows * positions * (width + LATENT),
        bytes_accessed=2 * positions * width,
        transcendentals=rows * positions,
    )

    lent, rows_q, keys = pl.pallas_call(
        lend,
        in_specs=[anywhere()] * 4,
        out_specs=[whole()] * 3,
        out_shape=[
            triple,
            pltpu.VMEM((rows, width), jnp.bfloat16),
            pltpu.VMEM((width, positions), jnp.bfloat16),
        ],
        scratch_shapes=[
            pltpu.VMEM(query.shape, jnp.bfloat16),
            pltpu.VMEM((rows, width), jnp.bfloat16),
            pltpu.VMEM((width, positions), jnp.bfloat16),
            score,
            *limits,
            pltpu.SemaphoreType.DMA((3,)),
            pltpu.SemaphoreType.DMA((parts,)),
            pltpu.SemaphoreType.DMA((parts,)),
        ],
        compiler_params=pltpu.CompilerParams(vmem_limit_bytes=32 * 2**20),
        cost_estimate=cost,
        name="lend",
    )(lengths, offsets, query, cache)
    lent = lax.ppermute(lent, CORE, swap)
    kept = pl.pallas_call(
        keep,
        in_specs=[anywhere(), anywhere(), whole(), whole()],
        out_specs=whole(),
        out_shape=triple,
        scratch_shapes=[score, *limits, pltpu.SemaphoreType.DMA((2,))],
        compiler_params=pltpu.CompilerParams(vmem_limit_bytes=32 * 2**20),
        cost_estimate=cost,
        name="keep",
    )(lengths, offsets, rows_q, keys)
    packed = pl.pallas_call(
        merge,
        in_specs=[whole()] * 2,
        out_specs=whole(),
        out_shape=pltpu.VMEM((rows, LATENT + LANES), jnp.int16),
        compiler_params=pltpu.CompilerParams(vmem_limit_bytes=8 * 2**20),
        name="merge",
    )(kept, lent)
    packed = packed.reshape(chips, rows // chips, LATENT + LANES)
    packed = lax.all_to_all(packed, CHIPS, 0, 0, tiled=True)
    copies = pl.pallas_call(
        finish,
        in_specs=[whole()],
        out_specs=whole(),
        out_shape=pltpu.VMEM((chips, rows // chips, LATENT), jnp.bfloat16),
        compiler_params=pltpu.CompilerParams(vmem_limit_bytes=8 * 2**20),
        name="finish",
    )(packed)
    mine = lax.all_to_all(copies, CHIPS, 0, 0, tiled=True).reshape(rows, LATENT)
    other = lax.ppermute(mine, CORE, swap)
    first = lax.axis_index(CORE) == 0
    both = jnp.where(first, jnp.stack([mine, other]), jnp.stack([other, mine]))
    return both.reshape(requests, qtokens, heads, LATENT)


def solution(mesh):
    torus = Mesh(mesh.devices.reshape(4, 4, 4, 2), SEQ)
    in_specs = (P(), P(None, SEQ, None), P(), P())
    return jax.shard_map(
        on_device, mesh=torus, in_specs=in_specs, out_specs=P(), check_vma=False
    )
```

```python
import functools

import jax
import jax.numpy as jnp
from jax import lax
from jax.experimental import pallas as pl
from jax.experimental.pallas import tpu as pltpu
from jax.sharding import Mesh
from jax.sharding import PartitionSpec as P

LATENT = 512
CHIPS = ("seq_0", "seq_1", "seq_2")
CORE = "seq_3"
SEQ = (*CHIPS, CORE)
LANES = 128
SUBLANES = 8
HIDDEN = -1e30
LOG2_SCALE = 192.0 ** (-0.5) * 1.4426950408889634
CHUNK = 1024
STEPS = 32000.0
FINE = 32768.0
F32 = jnp.float32
whole = functools.partial(pl.BlockSpec, memory_space=pltpu.VMEM)
anywhere = functools.partial(pl.BlockSpec, memory_space=pltpu.HBM)


def scores(rows_q, keys, limits, score, peaks, ready):
    rows, positions = score.shape
    qtokens = limits.shape[0] // SUBLANES
    heads = rows // qtokens
    lane = lax.broadcasted_iota(jnp.int32, (heads, CHUNK), 1)
    peaks[...] = jnp.full((rows, LANES), HIDDEN, F32)
    for j in range(positions // CHUNK):
        part = slice(j * CHUNK, (j + 1) * CHUNK)
        ready(j)
        product = jnp.dot(rows_q[:, :LATENT], keys[:LATENT, part], preferred_element_type=F32)
        product += jnp.dot(rows_q[:, LATENT:], keys[LATENT:, part], preferred_element_type=F32)
        for t in range(qtokens):
            r = slice(t * heads, (t + 1) * heads)
            limit = limits[t * SUBLANES : t * SUBLANES + 1, :1] - j * CHUNK
            seen = jnp.where(lane < limit, product[r], HIDDEN)
            score[r, part] = seen
            top = peaks[r, :]
            for u in range(CHUNK // LANES):
                top = jnp.maximum(top, seen[:, u * LANES : (u + 1) * LANES])
            peaks[r, :] = top


def values(score, keys, peak, out):
    rows, positions = score.shape
    base = jnp.where(peak < 0.1 * HIDDEN, 0.0, peak)
    total = jnp.zeros((rows, LANES), F32)
    for j in range(positions // CHUNK):
        part = slice(j * CHUNK, (j + 1) * CHUNK)
        weight = jnp.exp2((score[:, part] - base) * LOG2_SCALE)
        for u in range(CHUNK // LANES):
            total = total + weight[:, u * LANES : (u + 1) * LANES]
        value = lax.dot_general(
            weight.astype(jnp.bfloat16),
            keys[:LATENT, part],
            (((1,), (1,)), ((), ())),
            preferred_element_type=F32,
        )
        if j == 0:
            out[...] = value
        else:
            out[...] += value
    return jnp.sum(total, axis=1, keepdims=True)


def lend(lengths, offsets, queries, cache, triple, next_q, next_keys, next_limits, query, rows_q, keys, score, limits, lens, offs, sems, key_sems, next_sems):
    positions = keys.shape[1]
    qtokens, _, heads = query.shape[1:]
    own = lax.axis_index(CORE)
    other = 1 - own
    start = lax.axis_index(SEQ) * positions

    def key_copy(request, into, own_sems, j):
        part = pl.ds(j * CHUNK, CHUNK)
        return pltpu.make_async_copy(cache.at[request, :, part], into.at[:, part], own_sems.at[j])

    parts = range(positions // CHUNK)
    first = [key_copy(other, keys, key_sems, j) for j in parts]
    later = [key_copy(own, next_keys, next_sems, j) for j in parts]
    query_copy = pltpu.make_async_copy(queries.at[other], query.at[0], sems.at[0])
    later_query = pltpu.make_async_copy(queries.at[own], query.at[1], sems.at[1])
    scalars = [
        pltpu.make_async_copy(lengths, lens, sems.at[2]),
        pltpu.make_async_copy(offsets, offs, sems.at[3]),
    ]
    for copy in (query_copy, first[0], *scalars, *first[1:], later_query, *later):
        copy.start()
    query_copy.wait()
    for t in range(qtokens):
        rows_q[t * heads : (t + 1) * heads, :] = query[0, t].T
    for copy in scalars:
        copy.wait()
    for request, into in ((other, limits), (own, next_limits)):
        for t in range(qtokens):
            limit = lens[request] - qtokens + 1 + offs[request, t] - start
            into[t * SUBLANES : (t + 1) * SUBLANES, :] = jnp.full((SUBLANES, LANES), limit, jnp.int32)
    stats = triple.at[:, LATENT:]
    scores(rows_q, keys, limits, score, stats, lambda j: first[j].wait())
    later_query.wait()
    for t in range(qtokens):
        next_q[t * heads : (t + 1) * heads, :] = query[1, t].T
    for copy in later:
        copy.wait()
    peak = jnp.max(stats[...], axis=1, keepdims=True)
    total = values(score, keys, peak, triple.at[:, :LATENT])
    left = lax.broadcasted_iota(jnp.int32, stats.shape, 1) < LANES // 2
    stats[...] = jnp.where(left, peak, total)


def look(rows_q, keys, limits, score, peaks):
    scores(rows_q, keys, limits, score, peaks, lambda j: None)


def in_parts(x):
    whole_part = jnp.round(x)
    rest = (x - whole_part) * FINE
    middle = jnp.round(rest)
    return [whole_part, middle, jnp.round((rest - middle) * FINE)]


def from_parts(stats, at):
    a, b, c = (stats[..., at + i : at + i + 1] for i in range(3))
    return a + (b + c * (1.0 / FINE)) * (1.0 / FINE)


def keep(score, peaks, keys, lent, packed, kept):
    half = LATENT + LANES // 2
    peak_a, peak_b = jnp.max(peaks[...], axis=1, keepdims=True), lent[:, LATENT : LATENT + 1]
    total_a = values(score, keys, peak_a, kept)
    peak = jnp.maximum(peak_a, peak_b)
    factor_a = jnp.exp2((peak_a - peak) * LOG2_SCALE)
    factor_b = jnp.exp2((peak_b - peak) * LOG2_SCALE)
    total = factor_a * total_a + factor_b * lent[:, half : half + 1]
    both = factor_a * kept[...] + factor_b * lent[:, :LATENT]
    largest = jnp.max(jnp.abs(both), axis=1, keepdims=True)
    largest = jnp.where(largest > 0.0, largest, 1.0)
    packed[:, :LATENT] = jnp.round(both * (STEPS / largest)).astype(jnp.int32).astype(jnp.int16)
    level = jnp.maximum(peak * LOG2_SCALE, -STEPS)
    numbers = [*in_parts(level), *in_parts(total), *in_parts(jnp.log2(largest))]
    lane = lax.broadcasted_iota(jnp.int32, (kept.shape[0], LANES), 1)
    stats = jnp.zeros(lane.shape, F32)
    for i, number in enumerate(numbers):
        stats = jnp.where(lane == i, number, stats)
    packed[:, LATENT:] = stats.astype(jnp.int32).astype(jnp.int16)


def finish(packed, copies):
    chips, rows, _ = packed.shape
    stats = packed[:, :, LATENT:].astype(jnp.int32).astype(F32)
    level = from_parts(stats, 0)
    level = level - jnp.max(level, axis=0, keepdims=True)
    lower = jnp.sum(jnp.exp2(level) * from_parts(stats, 3), axis=0)
    factor = jnp.exp2(level + from_parts(stats, 6)) * (1.0 / STEPS)
    values = packed[:, :, :LATENT].astype(jnp.int32).astype(F32)
    upper = jnp.sum(factor * values, axis=0)
    final = (upper / lower).astype(jnp.bfloat16)
    copies[...] = jnp.broadcast_to(final[None], copies.shape)


def place_own(rows, out, sem):
    copy = pltpu.make_async_copy(rows, out.at[lax.axis_index(CORE)], sem)
    copy.start()
    copy.wait()


def place_other(rows, half_done, out, sem):
    copy = pltpu.make_async_copy(rows, out.at[1 - lax.axis_index(CORE)], sem)
    copy.start()
    copy.wait()


def on_device(queries, latent_cache, lengths, offsets):
    requests, qtokens, heads, width = queries.shape
    positions = latent_cache.shape[1]
    rows = qtokens * heads
    chips = lax.axis_size(CHIPS)
    in_hbm = lambda a: pltpu.with_memory_space_constraint(a, pltpu.HBM)
    query = in_hbm(jnp.transpose(queries, (0, 1, 3, 2)))
    cache = in_hbm(jnp.transpose(latent_cache, (0, 2, 1)))
    lengths, offsets = in_hbm(lengths), in_hbm(offsets)
    swap = [(0, 1), (1, 0)]
    parts = positions // CHUNK
    score = pltpu.VMEM((rows, positions), F32)
    line = pltpu.VMEM((rows, width), jnp.bfloat16)
    key = pltpu.VMEM((width, positions), jnp.bfloat16)
    limit = pltpu.VMEM((qtokens * SUBLANES, LANES), jnp.int32)
    out = jax.ShapeDtypeStruct((requests, rows, LATENT), jnp.bfloat16)

    def cost(depth):
        return pl.CostEstimate(
            flops=2 * rows * positions * depth,
            bytes_accessed=2 * positions * width,
            transcendentals=rows * positions,
        )

    lent, rows_q, keys, limits = pl.pallas_call(
        lend,
        in_specs=[anywhere()] * 4,
        out_specs=[whole()] * 4,
        out_shape=[pltpu.VMEM((rows, LATENT + LANES), F32), line, key, limit],
        scratch_shapes=[
            pltpu.VMEM(query.shape, jnp.bfloat16),
            line,
            key,
            score,
            limit,
            pltpu.SMEM(lengths.shape, jnp.int32),
            pltpu.SMEM(offsets.shape, jnp.int32),
            pltpu.SemaphoreType.DMA((4,)),
            pltpu.SemaphoreType.DMA((parts,)),
            pltpu.SemaphoreType.DMA((parts,)),
        ],
        compiler_params=pltpu.CompilerParams(vmem_limit_bytes=32 * 2**20),
        cost_estimate=cost(width + LATENT),
        name="lend",
    )(lengths, offsets, query, cache)
    lent = lax.ppermute(lent, CORE, swap)
    score, peaks = pl.pallas_call(
        look,
        in_specs=[whole()] * 3,
        out_specs=[whole()] * 2,
        out_shape=[score, pltpu.VMEM((rows, LANES), F32)],
        compiler_params=pltpu.CompilerParams(vmem_limit_bytes=16 * 2**20),
        cost_estimate=cost(width),
        name="look",
    )(rows_q, keys, limits)
    packed = pl.pallas_call(
        keep,
        in_specs=[whole()] * 4,
        out_specs=whole(),
        out_shape=pltpu.VMEM((rows, LATENT + LANES), jnp.int16),
        scratch_shapes=[pltpu.VMEM((rows, LATENT), F32)],
        compiler_params=pltpu.CompilerParams(vmem_limit_bytes=16 * 2**20),
        cost_estimate=cost(LATENT),
        name="keep",
    )(score, peaks, keys, lent)
    packed = packed.reshape(chips, rows // chips, LATENT + LANES)
    packed = lax.all_to_all(packed, CHIPS, 0, 0, tiled=True)
    copies = pl.pallas_call(
        finish,
        in_specs=[whole()],
        out_specs=whole(),
        out_shape=pltpu.VMEM((chips, rows // chips, LATENT), jnp.bfloat16),
        compiler_params=pltpu.CompilerParams(vmem_limit_bytes=8 * 2**20),
        name="finish",
    )(packed)
    mine = lax.all_to_all(copies, CHIPS, 0, 0, tiled=True).reshape(rows, LATENT)
    other = lax.ppermute(mine, CORE, swap)
    both = pl.pallas_call(
        place_own,
        in_specs=[whole()],
        out_specs=anywhere(),
        out_shape=out,
        scratch_shapes=[pltpu.SemaphoreType.DMA(())],
        compiler_params=pltpu.CompilerParams(vmem_limit_bytes=2**20),
        cost_estimate=pl.CostEstimate(flops=10**7, bytes_accessed=4 * rows * LATENT, transcendentals=0),
        name="place_own",
    )(mine)
    both = pl.pallas_call(
        place_other,
        in_specs=[whole(), anywhere()],
        out_specs=anywhere(),
        out_shape=out,
        input_output_aliases={1: 0},
        scratch_shapes=[pltpu.SemaphoreType.DMA(())],
        compiler_params=pltpu.CompilerParams(vmem_limit_bytes=2**20),
        name="place_other",
    )(other, both)
    return both.reshape(requests, qtokens, heads, LATENT)


def solution(mesh):
    torus = Mesh(mesh.devices.reshape(4, 4, 4, 2), SEQ)
    in_specs = (P(), P(None, SEQ, None), P(), P())
    return jax.shard_map(
        on_device, mesh=torus, in_specs=in_specs, out_specs=P(), check_vma=False
    )
```

```python
import functools

import jax
import jax.numpy as jnp
from jax import lax
from jax.experimental import pallas as pl
from jax.experimental.pallas import tpu as pltpu
from jax.sharding import Mesh
from jax.sharding import PartitionSpec as P

LATENT = 512
CHIPS = ("seq_0", "seq_1", "seq_2")
CORE = "seq_3"
SEQ = (*CHIPS, CORE)
LANES = 128
SUBLANES = 8
HIDDEN = -1e30
LOG2_SCALE = 192.0 ** (-0.5) * 1.4426950408889634
CHUNK = 1024
FIRST = 1024
STEP = 256
STEPS = 32000.0
FINE = 32768.0
F32 = jnp.float32
whole = functools.partial(pl.BlockSpec, memory_space=pltpu.VMEM)
anywhere = functools.partial(pl.BlockSpec, memory_space=pltpu.HBM)


def scores(rows_q, keys, limits, score, peaks, spans, ready):
    rows = score.shape[0]
    qtokens = limits.shape[0] // SUBLANES
    heads = rows // qtokens
    peaks[...] = jnp.full((rows, LANES), HIDDEN, F32)
    for j, (begin, size) in enumerate(spans):
        part = slice(begin, begin + size)
        lane = lax.broadcasted_iota(jnp.int32, (heads, size), 1)
        ready(j)
        product = jnp.dot(rows_q[:, :LATENT], keys[:LATENT, part], preferred_element_type=F32)
        product += jnp.dot(rows_q[:, LATENT:], keys[LATENT:, part], preferred_element_type=F32)
        for t in range(qtokens):
            r = slice(t * heads, (t + 1) * heads)
            limit = limits[t * SUBLANES : t * SUBLANES + 1, :1] - begin
            seen = jnp.where(lane < limit, product[r], HIDDEN)
            score[r, part] = seen
            top = peaks[r, :]
            for u in range(size // LANES):
                top = jnp.maximum(top, seen[:, u * LANES : (u + 1) * LANES])
            peaks[r, :] = top


def values(score, keys, peak, out):
    rows, positions = score.shape
    base = jnp.broadcast_to(jnp.where(peak < 0.1 * HIDDEN, 0.0, peak), (rows, LANES))
    total = jnp.zeros((rows, LANES), F32)

    def weights(j, base, total):
        cut = []
        for u in range(j * STEP, (j + 1) * STEP, LANES):
            weight = jnp.exp2((score[:, u : u + LANES] - base) * LOG2_SCALE)
            total = total + weight
            cut.append(weight.astype(jnp.bfloat16))
        return jnp.concatenate(cut, axis=1), total

    weight, total = weights(0, base, total)
    for j in range(positions // STEP):
        value = lax.dot_general(
            weight,
            keys[:LATENT, j * STEP : (j + 1) * STEP],
            (((1,), (1,)), ((), ())),
            preferred_element_type=F32,
        )
        if j == 0:
            out[...] = value
        else:
            out[...] += value
        if (j + 1) * STEP < positions:
            weight, total = weights(j + 1, base + value[:, :LANES] * 0.0, total)
    return jnp.sum(total, axis=1, keepdims=True)


def lend(lengths, offsets, queries, cache, triple, next_q, next_keys, next_limits, query, rows_q, keys, score, limits, lens, offs, sems, key_sems, next_sems, *, spans):
    positions = keys.shape[1]
    qtokens, _, heads = query.shape[1:]
    own = lax.axis_index(CORE)
    other = 1 - own
    start = lax.axis_index(SEQ) * positions

    def key_copy(request, into, own_sems, j):
        part = pl.ds(*spans[j])
        return pltpu.make_async_copy(cache.at[request, :, part], into.at[:, part], own_sems.at[j])

    parts = range(len(spans))
    first = [key_copy(other, keys, key_sems, j) for j in parts]
    later = [key_copy(own, next_keys, next_sems, j) for j in parts]
    query_copy = pltpu.make_async_copy(queries.at[other], query.at[0], sems.at[0])
    later_query = pltpu.make_async_copy(queries.at[own], query.at[1], sems.at[1])
    scalars = [
        pltpu.make_async_copy(lengths, lens, sems.at[2]),
        pltpu.make_async_copy(offsets, offs, sems.at[3]),
    ]
    for copy in (query_copy, first[0], *scalars, *first[1:], later_query, *later):
        copy.start()
    query_copy.wait()
    for t in range(qtokens):
        rows_q[t * heads : (t + 1) * heads, :] = query[0, t].T
    for copy in scalars:
        copy.wait()
    for request, into in ((other, limits), (own, next_limits)):
        for t in range(qtokens):
            limit = lens[request] - qtokens + 1 + offs[request, t] - start
            into[t * SUBLANES : (t + 1) * SUBLANES, :] = jnp.full((SUBLANES, LANES), limit, jnp.int32)
    stats = triple.at[:, LATENT : LATENT + LANES]
    scores(rows_q, keys, limits, score, stats, spans, lambda j: first[j].wait())
    later_query.wait()
    for t in range(qtokens):
        next_q[t * heads : (t + 1) * heads, :] = query[1, t].T
    for copy in later:
        copy.wait()
    peak = jnp.max(stats[...], axis=1, keepdims=True)
    total = values(score, keys, peak, triple.at[:, :LATENT])
    stats[...] = jnp.broadcast_to(peak, stats.shape)
    triple[:, LATENT + LANES :] = jnp.broadcast_to(total, stats.shape)


def look(rows_q, keys, limits, score, peaks):
    positions = score.shape[1]
    spans = [(i, CHUNK) for i in range(0, positions, CHUNK)]
    scores(rows_q, keys, limits, score, peaks, spans, lambda j: None)


def from_parts(stats, at):
    a, b, c = (stats[..., at + i : at + i + 1] for i in range(3))
    return a + (b + c * (1.0 / FINE)) * (1.0 / FINE)


def keep(score, peaks, keys, lent, packed, kept, scaled):
    peak_a, peak_b = jnp.max(peaks[...], axis=1, keepdims=True), lent[:, LATENT : LATENT + LANES]
    peak = jnp.maximum(peak_a, peak_b)
    factor_a = jnp.exp2((peak_a - peak) * LOG2_SCALE)
    factor_b = jnp.exp2((peak_b - peak) * LOG2_SCALE)
    total = factor_b * lent[:, LATENT + LANES :]
    blocks = range(0, LATENT, LANES)
    for u in blocks:
        scaled[:, u : u + LANES] = factor_b * lent[:, u : u + LANES]
    total = total + factor_a * values(score, keys, peak_a, kept)
    both = [factor_a * kept[:, u : u + LANES] + scaled[:, u : u + LANES] for u in blocks]
    sizes = [jnp.abs(x) for x in both]
    largest = jnp.maximum(jnp.maximum(sizes[0], sizes[1]), jnp.maximum(sizes[2], sizes[3]))
    largest = jnp.max(largest, axis=1, keepdims=True)
    largest = jnp.broadcast_to(jnp.where(largest > 0.0, largest, 1.0), peak.shape)
    steps = STEPS / largest
    for u, x in zip(blocks, both):
        packed[:, u : u + LANES] = jnp.round(x * steps).astype(jnp.int32).astype(jnp.int16)
    lane = lax.broadcasted_iota(jnp.int32, peak.shape, 1)
    level = jnp.maximum(peak * LOG2_SCALE, -STEPS)
    number = jnp.where(lane < 3, level, jnp.where(lane < 6, total, jnp.log2(largest)))
    whole_part = jnp.round(number)
    rest = (number - whole_part) * FINE
    middle = jnp.round(rest)
    last = jnp.round((rest - middle) * FINE)
    digit = lane % 3
    stats = jnp.where(digit == 0, whole_part, jnp.where(digit == 1, middle, last))
    packed[:, LATENT:] = stats.astype(jnp.int32).astype(jnp.int16)


def finish(packed, copies):
    chips, rows, _ = packed.shape
    stats = packed[:, :, LATENT:].astype(jnp.int32).astype(F32)
    level = from_parts(stats, 0)
    level = level - jnp.max(level, axis=0, keepdims=True)
    lower = jnp.sum(jnp.exp2(level) * from_parts(stats, 3), axis=0)
    factor = jnp.exp2(level + from_parts(stats, 6)) * (1.0 / STEPS)
    values = packed[:, :, :LATENT].astype(jnp.int32).astype(F32)
    upper = jnp.sum(factor * values, axis=0)
    final = (upper / lower).astype(jnp.bfloat16)
    copies[...] = jnp.broadcast_to(final[None], copies.shape)


def place_own(rows, out, sem):
    copy = pltpu.make_async_copy(rows, out.at[lax.axis_index(CORE)], sem)
    copy.start()
    copy.wait()


def place_other(rows, half_done, out, sem):
    copy = pltpu.make_async_copy(rows, out.at[1 - lax.axis_index(CORE)], sem)
    copy.start()
    copy.wait()


def on_device(queries, latent_cache, lengths, offsets):
    requests, qtokens, heads, width = queries.shape
    positions = latent_cache.shape[1]
    rows = qtokens * heads
    chips = lax.axis_size(CHIPS)
    in_hbm = lambda a: pltpu.with_memory_space_constraint(a, pltpu.HBM)
    query = in_hbm(jnp.transpose(queries, (0, 1, 3, 2)))
    cache = in_hbm(jnp.transpose(latent_cache, (0, 2, 1)))
    lengths, offsets = in_hbm(lengths), in_hbm(offsets)
    swap = [(0, 1), (1, 0)]
    spans = [(0, FIRST), (FIRST, positions - FIRST)]
    score = pltpu.VMEM((rows, positions), F32)
    line = pltpu.VMEM((rows, width), jnp.bfloat16)
    key = pltpu.VMEM((width, positions), jnp.bfloat16)
    limit = pltpu.VMEM((qtokens * SUBLANES, LANES), jnp.int32)
    out = jax.ShapeDtypeStruct((requests, rows, LATENT), jnp.bfloat16)

    def cost(depth):
        return pl.CostEstimate(
            flops=2 * rows * positions * depth,
            bytes_accessed=2 * positions * width,
            transcendentals=rows * positions,
        )

    lent, rows_q, keys, limits = pl.pallas_call(
        functools.partial(lend, spans=spans),
        in_specs=[anywhere()] * 4,
        out_specs=[whole()] * 4,
        out_shape=[pltpu.VMEM((rows, LATENT + 2 * LANES), F32), line, key, limit],
        scratch_shapes=[
            pltpu.VMEM(query.shape, jnp.bfloat16),
            line,
            key,
            score,
            limit,
            pltpu.SMEM(lengths.shape, jnp.int32),
            pltpu.SMEM(offsets.shape, jnp.int32),
            pltpu.SemaphoreType.DMA((4,)),
            pltpu.SemaphoreType.DMA((len(spans),)),
            pltpu.SemaphoreType.DMA((len(spans),)),
        ],
        compiler_params=pltpu.CompilerParams(vmem_limit_bytes=32 * 2**20),
        cost_estimate=cost(width + LATENT),
        name="lend",
    )(lengths, offsets, query, cache)
    lent = lax.ppermute(lent, CORE, swap)
    score, peaks = pl.pallas_call(
        look,
        in_specs=[whole()] * 3,
        out_specs=[whole()] * 2,
        out_shape=[score, pltpu.VMEM((rows, LANES), F32)],
        compiler_params=pltpu.CompilerParams(vmem_limit_bytes=16 * 2**20),
        cost_estimate=cost(width),
        name="look",
    )(rows_q, keys, limits)
    packed = pl.pallas_call(
        keep,
        in_specs=[whole()] * 4,
        out_specs=whole(),
        out_shape=pltpu.VMEM((rows, LATENT + LANES), jnp.int16),
        scratch_shapes=[pltpu.VMEM((rows, LATENT), F32)] * 2,
        compiler_params=pltpu.CompilerParams(vmem_limit_bytes=16 * 2**20),
        cost_estimate=cost(LATENT),
        name="keep",
    )(score, peaks, keys, lent)
    packed = packed.reshape(chips, rows // chips, LATENT + LANES)
    packed = lax.all_to_all(packed, CHIPS, 0, 0, tiled=True)
    copies = pl.pallas_call(
        finish,
        in_specs=[whole()],
        out_specs=whole(),
        out_shape=pltpu.VMEM((chips, rows // chips, LATENT), jnp.bfloat16),
        compiler_params=pltpu.CompilerParams(vmem_limit_bytes=8 * 2**20),
        name="finish",
    )(packed)
    mine = lax.all_to_all(copies, CHIPS, 0, 0, tiled=True).reshape(rows, LATENT)
    other = lax.ppermute(mine, CORE, swap)
    both = pl.pallas_call(
        place_own,
        in_specs=[whole()],
        out_specs=anywhere(),
        out_shape=out,
        scratch_shapes=[pltpu.SemaphoreType.DMA(())],
        compiler_params=pltpu.CompilerParams(vmem_limit_bytes=2**20),
        cost_estimate=pl.CostEstimate(flops=10**7, bytes_accessed=4 * rows * LATENT, transcendentals=0),
        name="place_own",
    )(mine)
    both = pl.pallas_call(
        place_other,
        in_specs=[whole(), anywhere()],
        out_specs=anywhere(),
        out_shape=out,
        input_output_aliases={1: 0},
        scratch_shapes=[pltpu.SemaphoreType.DMA(())],
        compiler_params=pltpu.CompilerParams(vmem_limit_bytes=2**20),
        name="place_other",
    )(other, both)
    return both.reshape(requests, qtokens, heads, LATENT)


def solution(mesh):
    torus = Mesh(mesh.devices.reshape(4, 4, 4, 2), SEQ)
    in_specs = (P(), P(None, SEQ, None), P(), P())
    return jax.shard_map(
        on_device, mesh=torus, in_specs=in_specs, out_specs=P(), check_vma=False
    )
```

```python
import functools

import jax
import jax.numpy as jnp
from jax import lax
from jax.experimental import pallas as pl
from jax.experimental.pallas import tpu as pltpu
from jax.sharding import Mesh
from jax.sharding import PartitionSpec as P

LATENT = 512
CHIPS = ("seq_0", "seq_1", "seq_2")
CORE = "seq_3"
SEQ = (*CHIPS, CORE)
LANES = 128
SUBLANES = 8
HIDDEN = -1e30
LOG2_SCALE = 192.0 ** (-0.5) * 1.4426950408889634
CHUNK = 1024
FIRST = 1024
STEP = 256
STEPS = 32000.0
FINE = 32768.0
F32 = jnp.float32
whole = functools.partial(pl.BlockSpec, memory_space=pltpu.VMEM)
anywhere = functools.partial(pl.BlockSpec, memory_space=pltpu.HBM)


def scores(rows_q, keys, limits, score, peaks, spans, ready):
    rows = score.shape[0]
    qtokens = limits.shape[0] // SUBLANES
    heads = rows // qtokens
    peaks[...] = jnp.full((rows, LANES), HIDDEN, F32)
    for j, (begin, size) in enumerate(spans):
        part = slice(begin, begin + size)
        lane = lax.broadcasted_iota(jnp.int32, (heads, size), 1)
        ready(j)
        product = jnp.dot(rows_q[:, :LATENT], keys[:LATENT, part], preferred_element_type=F32)
        product += jnp.dot(rows_q[:, LATENT:], keys[LATENT:, part], preferred_element_type=F32)
        for t in range(qtokens):
            r = slice(t * heads, (t + 1) * heads)
            limit = limits[t * SUBLANES : t * SUBLANES + 1, :1] - begin
            seen = jnp.where(lane < limit, product[r], HIDDEN)
            score[r, part] = seen
            top = peaks[r, :]
            for u in range(size // LANES):
                top = jnp.maximum(top, seen[:, u * LANES : (u + 1) * LANES])
            peaks[r, :] = top


def values(score, keys, peak, out):
    rows, positions = score.shape
    base = jnp.broadcast_to(jnp.where(peak < 0.1 * HIDDEN, 0.0, peak), (rows, LANES))
    total = jnp.zeros((rows, LANES), F32)

    def weights(j, base, total):
        cut = []
        for u in range(j * STEP, (j + 1) * STEP, LANES):
            weight = jnp.exp2((score[:, u : u + LANES] - base) * LOG2_SCALE)
            total = total + weight
            cut.append(weight.astype(jnp.bfloat16))
        return jnp.concatenate(cut, axis=1), total

    weight, total = weights(0, base, total)
    for j in range(positions // STEP):
        value = lax.dot_general(
            weight,
            keys[:LATENT, j * STEP : (j + 1) * STEP],
            (((1,), (1,)), ((), ())),
            preferred_element_type=F32,
        )
        if j == 0:
            out[...] = value
        else:
            out[...] += value
        if (j + 1) * STEP < positions:
            weight, total = weights(j + 1, base + value[:, :LANES] * 0.0, total)
    return jnp.sum(total, axis=1, keepdims=True)


def lend(lengths, offsets, queries, cache, triple, next_q, next_keys, next_limits, query, rows_q, keys, score, limits, lens, offs, sems, key_sems, next_sems, *, spans):
    positions = keys.shape[1]
    qtokens, _, heads = query.shape[1:]
    own = lax.axis_index(CORE)
    other = 1 - own
    start = lax.axis_index(SEQ) * positions

    def key_copy(request, into, own_sems, j):
        part = pl.ds(*spans[j])
        return pltpu.make_async_copy(cache.at[request, :, part], into.at[:, part], own_sems.at[j])

    parts = range(len(spans))
    first = [key_copy(other, keys, key_sems, j) for j in parts]
    later = [key_copy(own, next_keys, next_sems, j) for j in parts]
    query_copy = pltpu.make_async_copy(queries.at[other], query.at[0], sems.at[0])
    later_query = pltpu.make_async_copy(queries.at[own], query.at[1], sems.at[1])
    scalars = [
        pltpu.make_async_copy(lengths, lens, sems.at[2]),
        pltpu.make_async_copy(offsets, offs, sems.at[3]),
    ]
    for copy in (query_copy, first[0], *scalars, *first[1:], later_query, *later):
        copy.start()
    query_copy.wait()
    for t in range(qtokens):
        rows_q[t * heads : (t + 1) * heads, :] = query[0, t].T
    for copy in scalars:
        copy.wait()
    for request, into in ((other, limits), (own, next_limits)):
        last = jnp.int32(0)
        for t in range(qtokens):
            limit = lens[request] - qtokens + 1 + offs[request, t] - start
            last = jnp.maximum(last, limit)
            into[t * SUBLANES : (t + 1) * SUBLANES, :] = jnp.full((SUBLANES, LANES), limit, jnp.int32)
        if into is limits:
            visible = last > 0
    peaks = triple.at[:, LATENT : LATENT + LANES]
    totals = triple.at[:, LATENT + LANES :]

    def fetch_next():
        later_query.wait()
        for t in range(qtokens):
            next_q[t * heads : (t + 1) * heads, :] = query[1, t].T
        for copy in later:
            copy.wait()

    @pl.when(visible)
    def _():
        scores(rows_q, keys, limits, score, peaks, spans, lambda j: first[j].wait())
        fetch_next()
        peak = jnp.max(peaks[...], axis=1, keepdims=True)
        total = values(score, keys, peak, triple.at[:, :LATENT])
        peaks[...] = jnp.broadcast_to(peak, peaks.shape)
        totals[...] = jnp.broadcast_to(total, totals.shape)

    @pl.when(jnp.logical_not(visible))
    def _():
        for copy in first:
            copy.wait()
        fetch_next()
        triple[...] = jnp.zeros(triple.shape, F32)
        peaks[...] = jnp.full(peaks.shape, HIDDEN, F32)


def look(rows_q, keys, limits, score, peaks):
    positions = score.shape[1]
    spans = [(i, CHUNK) for i in range(0, positions, CHUNK)]
    scores(rows_q, keys, limits, score, peaks, spans, lambda j: None)


def from_parts(stats, at):
    a, b, c = (stats[..., at + i : at + i + 1] for i in range(3))
    return a + (b + c * (1.0 / FINE)) * (1.0 / FINE)


def pack(both, peak, total, packed):
    sizes = [jnp.abs(x) for x in both]
    largest = jnp.maximum(jnp.maximum(sizes[0], sizes[1]), jnp.maximum(sizes[2], sizes[3]))
    largest = jnp.max(largest, axis=1, keepdims=True)
    largest = jnp.broadcast_to(jnp.where(largest > 0.0, largest, 1.0), peak.shape)
    steps = STEPS / largest
    for i, x in enumerate(both):
        packed[:, i * LANES : (i + 1) * LANES] = jnp.round(x * steps).astype(jnp.int32).astype(jnp.int16)
    lane = lax.broadcasted_iota(jnp.int32, peak.shape, 1)
    level = jnp.maximum(peak * LOG2_SCALE, -STEPS)
    number = jnp.where(lane < 3, level, jnp.where(lane < 6, total, jnp.log2(largest)))
    whole_part = jnp.round(number)
    rest = (number - whole_part) * FINE
    middle = jnp.round(rest)
    last = jnp.round((rest - middle) * FINE)
    digit = lane % 3
    stats = jnp.where(digit == 0, whole_part, jnp.where(digit == 1, middle, last))
    packed[:, LATENT:] = stats.astype(jnp.int32).astype(jnp.int16)


def keep(score, peaks, keys, lent, packed, kept, scaled):
    blocks = [slice(u, u + LANES) for u in range(0, LATENT, LANES)]
    peak_a, peak_b = jnp.max(peaks[...], axis=1, keepdims=True), lent[:, LATENT : LATENT + LANES]
    peak = jnp.maximum(peak_a, peak_b)
    factor_a = jnp.exp2((peak_a - peak) * LOG2_SCALE)
    factor_b = jnp.exp2((peak_b - peak) * LOG2_SCALE)
    total = factor_b * lent[:, LATENT + LANES :]
    for u in blocks:
        scaled[:, u] = factor_b * lent[:, u]
    total = total + factor_a * values(score, keys, peak_a, kept)
    pack([factor_a * kept[:, u] + scaled[:, u] for u in blocks], peak, total, packed)


def finish(packed, copies):
    chips, rows, _ = packed.shape
    stats = packed[:, :, LATENT:].astype(jnp.int32).astype(F32)
    level = from_parts(stats, 0)
    level = level - jnp.max(level, axis=0, keepdims=True)
    lower = jnp.sum(jnp.exp2(level) * from_parts(stats, 3), axis=0)
    factor = jnp.exp2(level + from_parts(stats, 6)) * (1.0 / STEPS)
    values = packed[:, :, :LATENT].astype(jnp.int32).astype(F32)
    upper = jnp.sum(factor * values, axis=0)
    final = (upper / lower).astype(jnp.bfloat16)
    copies[...] = jnp.broadcast_to(final[None], copies.shape)


def place_own(rows, out, sem):
    copy = pltpu.make_async_copy(rows, out.at[lax.axis_index(CORE)], sem)
    copy.start()
    copy.wait()


def place_other(rows, half_done, out, sem):
    copy = pltpu.make_async_copy(rows, out.at[1 - lax.axis_index(CORE)], sem)
    copy.start()
    copy.wait()


def on_device(queries, latent_cache, lengths, offsets):
    requests, qtokens, heads, width = queries.shape
    positions = latent_cache.shape[1]
    rows = qtokens * heads
    chips = lax.axis_size(CHIPS)
    in_hbm = lambda a: pltpu.with_memory_space_constraint(a, pltpu.HBM)
    query = in_hbm(jnp.transpose(queries, (0, 1, 3, 2)))
    cache = in_hbm(jnp.transpose(latent_cache, (0, 2, 1)))
    lengths, offsets = in_hbm(lengths), in_hbm(offsets)
    swap = [(0, 1), (1, 0)]
    spans = [(0, FIRST), (FIRST, positions - FIRST)]
    score = pltpu.VMEM((rows, positions), F32)
    line = pltpu.VMEM((rows, width), jnp.bfloat16)
    key = pltpu.VMEM((width, positions), jnp.bfloat16)
    limit = pltpu.VMEM((qtokens * SUBLANES, LANES), jnp.int32)
    out = jax.ShapeDtypeStruct((requests, rows, LATENT), jnp.bfloat16)

    def cost(depth):
        return pl.CostEstimate(
            flops=2 * rows * positions * depth,
            bytes_accessed=2 * positions * width,
            transcendentals=rows * positions,
        )

    lent, rows_q, keys, limits = pl.pallas_call(
        functools.partial(lend, spans=spans),
        in_specs=[anywhere()] * 4,
        out_specs=[whole()] * 4,
        out_shape=[pltpu.VMEM((rows, LATENT + 2 * LANES), F32), line, key, limit],
        scratch_shapes=[
            pltpu.VMEM(query.shape, jnp.bfloat16),
            line,
            key,
            score,
            limit,
            pltpu.SMEM(lengths.shape, jnp.int32),
            pltpu.SMEM(offsets.shape, jnp.int32),
            pltpu.SemaphoreType.DMA((4,)),
            pltpu.SemaphoreType.DMA((len(spans),)),
            pltpu.SemaphoreType.DMA((len(spans),)),
        ],
        compiler_params=pltpu.CompilerParams(vmem_limit_bytes=32 * 2**20),
        cost_estimate=cost(width + LATENT),
        name="lend",
    )(lengths, offsets, query, cache)
    lent = lax.ppermute(lent, CORE, swap)
    score, peaks = pl.pallas_call(
        look,
        in_specs=[whole()] * 3,
        out_specs=[whole()] * 2,
        out_shape=[score, pltpu.VMEM((rows, LANES), F32)],
        compiler_params=pltpu.CompilerParams(vmem_limit_bytes=16 * 2**20),
        cost_estimate=cost(width),
        name="look",
    )(rows_q, keys, limits)
    packed = pl.pallas_call(
        keep,
        in_specs=[whole()] * 4,
        out_specs=whole(),
        out_shape=pltpu.VMEM((rows, LATENT + LANES), jnp.int16),
        scratch_shapes=[pltpu.VMEM((rows, LATENT), F32)] * 2,
        compiler_params=pltpu.CompilerParams(vmem_limit_bytes=16 * 2**20),
        cost_estimate=cost(LATENT),
        name="keep",
    )(score, peaks, keys, lent)
    packed = packed.reshape(chips, rows // chips, LATENT + LANES)
    packed = lax.all_to_all(packed, CHIPS, 0, 0, tiled=True)
    copies = pl.pallas_call(
        finish,
        in_specs=[whole()],
        out_specs=whole(),
        out_shape=pltpu.VMEM((chips, rows // chips, LATENT), jnp.bfloat16),
        compiler_params=pltpu.CompilerParams(vmem_limit_bytes=8 * 2**20),
        name="finish",
    )(packed)
    mine = lax.all_to_all(copies, CHIPS, 0, 0, tiled=True).reshape(rows, LATENT)
    other = lax.ppermute(mine, CORE, swap)
    both = pl.pallas_call(
        place_own,
        in_specs=[whole()],
        out_specs=anywhere(),
        out_shape=out,
        scratch_shapes=[pltpu.SemaphoreType.DMA(())],
        compiler_params=pltpu.CompilerParams(vmem_limit_bytes=2**20),
        cost_estimate=pl.CostEstimate(flops=10**7, bytes_accessed=4 * rows * LATENT, transcendentals=0),
        name="place_own",
    )(mine)
    both = pl.pallas_call(
        place_other,
        in_specs=[whole(), anywhere()],
        out_specs=anywhere(),
        out_shape=out,
        input_output_aliases={1: 0},
        scratch_shapes=[pltpu.SemaphoreType.DMA(())],
        compiler_params=pltpu.CompilerParams(vmem_limit_bytes=2**20),
        name="place_other",
    )(other, both)
    return both.reshape(requests, qtokens, heads, LATENT)


def solution(mesh):
    torus = Mesh(mesh.devices.reshape(4, 4, 4, 2), SEQ)
    in_specs = (P(), P(None, SEQ, None), P(), P())
    return jax.shard_map(
        on_device, mesh=torus, in_specs=in_specs, out_specs=P(), check_vma=False
    )
```

```python
import functools

import jax
import jax.numpy as jnp
from jax import lax
from jax.experimental import pallas as pl
from jax.experimental.pallas import tpu as pltpu
from jax.sharding import Mesh
from jax.sharding import PartitionSpec as P

LATENT = 512
CHIPS = ("seq_0", "seq_1", "seq_2")
CORE = "seq_3"
SEQ = (*CHIPS, CORE)
LANES = 128
SUBLANES = 8
HIDDEN = -1e30
LOG2_SCALE = 192.0 ** (-0.5) * 1.4426950408889634
CHUNK = 1024
FIRST = 1024
STEP = 256
STEPS = 32000.0
FINE = 32768.0
F32 = jnp.float32
whole = functools.partial(pl.BlockSpec, memory_space=pltpu.VMEM)
anywhere = functools.partial(pl.BlockSpec, memory_space=pltpu.HBM)


def scores(rows_q, keys, limits, score, peaks, spans, ready):
    rows = score.shape[0]
    qtokens = limits.shape[0] // SUBLANES - 1
    heads = rows // qtokens
    peaks[...] = jnp.full((rows, LANES), HIDDEN, F32)
    for j, (begin, size) in enumerate(spans):
        part = slice(begin, begin + size)
        lane = lax.broadcasted_iota(jnp.int32, (heads, size), 1)
        ready(j)
        product = jnp.dot(rows_q[:, :LATENT], keys[:LATENT, part], preferred_element_type=F32)
        product += jnp.dot(rows_q[:, LATENT:], keys[LATENT:, part], preferred_element_type=F32)
        for t in range(qtokens):
            r = slice(t * heads, (t + 1) * heads)
            limit = limits[t * SUBLANES : t * SUBLANES + 1, :1] - begin
            seen = jnp.where(lane < limit, product[r], HIDDEN)
            score[r, part] = seen
            top = peaks[r, :]
            for u in range(size // LANES):
                top = jnp.maximum(top, seen[:, u * LANES : (u + 1) * LANES])
            peaks[r, :] = top


def values(score, keys, peak, out):
    rows, positions = score.shape
    base = jnp.broadcast_to(jnp.where(peak < 0.1 * HIDDEN, 0.0, peak), (rows, LANES))
    total = jnp.zeros((rows, LANES), F32)

    def weights(j, base, total):
        cut = []
        for u in range(j * STEP, (j + 1) * STEP, LANES):
            weight = jnp.exp2((score[:, u : u + LANES] - base) * LOG2_SCALE)
            total = total + weight
            cut.append(weight.astype(jnp.bfloat16))
        return jnp.concatenate(cut, axis=1), total

    weight, total = weights(0, base, total)
    for j in range(positions // STEP):
        value = lax.dot_general(
            weight,
            keys[:LATENT, j * STEP : (j + 1) * STEP],
            (((1,), (1,)), ((), ())),
            preferred_element_type=F32,
        )
        if j == 0:
            out[...] = value
        else:
            out[...] += value
        if (j + 1) * STEP < positions:
            weight, total = weights(j + 1, base + value[:, :LANES] * 0.0, total)
    return jnp.sum(total, axis=1, keepdims=True)


def lend(lengths, offsets, queries, cache, triple, next_q, next_keys, next_limits, query, rows_q, keys, score, limits, lens, offs, sems, key_sems, next_sems, *, spans):
    positions = keys.shape[1]
    qtokens, _, heads = query.shape[1:]
    own = lax.axis_index(CORE)
    other = 1 - own
    start = lax.axis_index(SEQ) * positions

    def key_copy(request, into, own_sems, j):
        part = pl.ds(*spans[j])
        return pltpu.make_async_copy(cache.at[request, :, part], into.at[:, part], own_sems.at[j])

    parts = range(len(spans))
    first = [key_copy(other, keys, key_sems, j) for j in parts]
    later = [key_copy(own, next_keys, next_sems, j) for j in parts]
    query_copy = pltpu.make_async_copy(queries.at[other], query.at[0], sems.at[0])
    later_query = pltpu.make_async_copy(queries.at[own], query.at[1], sems.at[1])
    scalars = [
        pltpu.make_async_copy(lengths, lens, sems.at[2]),
        pltpu.make_async_copy(offsets, offs, sems.at[3]),
    ]
    for copy in (query_copy, first[0], *scalars, *first[1:], later_query, *later):
        copy.start()
    query_copy.wait()
    for t in range(qtokens):
        rows_q[t * heads : (t + 1) * heads, :] = query[0, t].T
    for copy in scalars:
        copy.wait()
    for request, into in ((other, limits), (own, next_limits)):
        last = jnp.int32(0)
        for t in range(qtokens):
            limit = lens[request] - qtokens + 1 + offs[request, t] - start
            last = jnp.maximum(last, limit)
            into[t * SUBLANES : (t + 1) * SUBLANES, :] = jnp.full((SUBLANES, LANES), limit, jnp.int32)
        into[qtokens * SUBLANES :, :] = jnp.full((SUBLANES, LANES), last, jnp.int32)
        if into is limits:
            visible = last > 0
    peaks = triple.at[:, LATENT : LATENT + LANES]
    totals = triple.at[:, LATENT + LANES :]

    def fetch_next():
        later_query.wait()
        for t in range(qtokens):
            next_q[t * heads : (t + 1) * heads, :] = query[1, t].T
        for copy in later:
            copy.wait()

    @pl.when(visible)
    def _():
        scores(rows_q, keys, limits, score, peaks, spans, lambda j: first[j].wait())
        fetch_next()
        peak = jnp.max(peaks[...], axis=1, keepdims=True)
        total = values(score, keys, peak, triple.at[:, :LATENT])
        peaks[...] = jnp.broadcast_to(peak, peaks.shape)
        totals[...] = jnp.broadcast_to(total, totals.shape)

    @pl.when(jnp.logical_not(visible))
    def _():
        for copy in first:
            copy.wait()
        fetch_next()
        triple[...] = jnp.zeros(triple.shape, F32)
        peaks[...] = jnp.full(peaks.shape, HIDDEN, F32)


def look(rows_q, keys, limits, score, peaks):
    positions = score.shape[1]
    spans = [(i, CHUNK) for i in range(0, positions, CHUNK)]
    visible = jnp.max(limits[limits.shape[0] - 1 :, :1]) > 0

    @pl.when(visible)
    def _():
        scores(rows_q, keys, limits, score, peaks, spans, lambda j: None)

    @pl.when(jnp.logical_not(visible))
    def _():
        score[...] = jnp.full(score.shape, HIDDEN, F32)
        peaks[...] = jnp.full(peaks.shape, HIDDEN, F32)


def from_parts(stats, at):
    a, b, c = (stats[..., at + i : at + i + 1] for i in range(3))
    return a + (b + c * (1.0 / FINE)) * (1.0 / FINE)


def pack(both, peak, total, packed):
    sizes = [jnp.abs(x) for x in both]
    largest = jnp.maximum(jnp.maximum(sizes[0], sizes[1]), jnp.maximum(sizes[2], sizes[3]))
    largest = jnp.max(largest, axis=1, keepdims=True)
    largest = jnp.broadcast_to(jnp.where(largest > 0.0, largest, 1.0), peak.shape)
    steps = STEPS / largest
    for i, x in enumerate(both):
        packed[:, i * LANES : (i + 1) * LANES] = jnp.round(x * steps).astype(jnp.int32).astype(jnp.int16)
    lane = lax.broadcasted_iota(jnp.int32, peak.shape, 1)
    level = jnp.maximum(peak * LOG2_SCALE, -STEPS)
    number = jnp.where(lane < 3, level, jnp.where(lane < 6, total, jnp.log2(largest)))
    whole_part = jnp.round(number)
    rest = (number - whole_part) * FINE
    middle = jnp.round(rest)
    last = jnp.round((rest - middle) * FINE)
    digit = lane % 3
    stats = jnp.where(digit == 0, whole_part, jnp.where(digit == 1, middle, last))
    packed[:, LATENT:] = stats.astype(jnp.int32).astype(jnp.int16)


def keep(score, peaks, keys, lent, packed, kept, scaled):
    blocks = [slice(u, u + LANES) for u in range(0, LATENT, LANES)]
    peak_a, peak_b = jnp.max(peaks[...], axis=1, keepdims=True), lent[:, LATENT : LATENT + LANES]
    peak = jnp.maximum(peak_a, peak_b)
    factor_a = jnp.exp2((peak_a - peak) * LOG2_SCALE)
    factor_b = jnp.exp2((peak_b - peak) * LOG2_SCALE)
    total = factor_b * lent[:, LATENT + LANES :]
    for u in blocks:
        scaled[:, u] = factor_b * lent[:, u]
    total = total + factor_a * values(score, keys, peak_a, kept)
    pack([factor_a * kept[:, u] + scaled[:, u] for u in blocks], peak, total, packed)


def finish(packed, copies):
    chips, rows, _ = packed.shape
    stats = packed[:, :, LATENT:].astype(jnp.int32).astype(F32)
    level = from_parts(stats, 0)
    level = level - jnp.max(level, axis=0, keepdims=True)
    lower = jnp.sum(jnp.exp2(level) * from_parts(stats, 3), axis=0)
    factor = jnp.exp2(level + from_parts(stats, 6)) * (1.0 / STEPS)
    values = packed[:, :, :LATENT].astype(jnp.int32).astype(F32)
    upper = jnp.sum(factor * values, axis=0)
    final = (upper / lower).astype(jnp.bfloat16)
    copies[...] = jnp.broadcast_to(final[None], copies.shape)


def place_own(rows, out, sem):
    copy = pltpu.make_async_copy(rows, out.at[lax.axis_index(CORE)], sem)
    copy.start()
    copy.wait()


def place_other(rows, half_done, out, sem):
    copy = pltpu.make_async_copy(rows, out.at[1 - lax.axis_index(CORE)], sem)
    copy.start()
    copy.wait()


def on_device(queries, latent_cache, lengths, offsets):
    requests, qtokens, heads, width = queries.shape
    positions = latent_cache.shape[1]
    rows = qtokens * heads
    chips = lax.axis_size(CHIPS)
    in_hbm = lambda a: pltpu.with_memory_space_constraint(a, pltpu.HBM)
    query = in_hbm(jnp.transpose(queries, (0, 1, 3, 2)))
    cache = in_hbm(jnp.transpose(latent_cache, (0, 2, 1)))
    lengths, offsets = in_hbm(lengths), in_hbm(offsets)
    swap = [(0, 1), (1, 0)]
    spans = [(0, FIRST), (FIRST, positions - FIRST)]
    score = pltpu.VMEM((rows, positions), F32)
    line = pltpu.VMEM((rows, width), jnp.bfloat16)
    key = pltpu.VMEM((width, positions), jnp.bfloat16)
    limit = pltpu.VMEM(((qtokens + 1) * SUBLANES, LANES), jnp.int32)
    out = jax.ShapeDtypeStruct((requests, rows, LATENT), jnp.bfloat16)

    def cost(depth):
        return pl.CostEstimate(
            flops=2 * rows * positions * depth,
            bytes_accessed=2 * positions * width,
            transcendentals=rows * positions,
        )

    lent, rows_q, keys, limits = pl.pallas_call(
        functools.partial(lend, spans=spans),
        in_specs=[anywhere()] * 4,
        out_specs=[whole()] * 4,
        out_shape=[pltpu.VMEM((rows, LATENT + 2 * LANES), F32), line, key, limit],
        scratch_shapes=[
            pltpu.VMEM(query.shape, jnp.bfloat16),
            line,
            key,
            score,
            limit,
            pltpu.SMEM(lengths.shape, jnp.int32),
            pltpu.SMEM(offsets.shape, jnp.int32),
            pltpu.SemaphoreType.DMA((4,)),
            pltpu.SemaphoreType.DMA((len(spans),)),
            pltpu.SemaphoreType.DMA((len(spans),)),
        ],
        compiler_params=pltpu.CompilerParams(vmem_limit_bytes=32 * 2**20),
        cost_estimate=cost(width + LATENT),
        name="lend",
    )(lengths, offsets, query, cache)
    lent = lax.ppermute(lent, CORE, swap)
    score, peaks = pl.pallas_call(
        look,
        in_specs=[whole()] * 3,
        out_specs=[whole()] * 2,
        out_shape=[score, pltpu.VMEM((rows, LANES), F32)],
        compiler_params=pltpu.CompilerParams(vmem_limit_bytes=16 * 2**20),
        cost_estimate=cost(width),
        name="look",
    )(rows_q, keys, limits)
    packed = pl.pallas_call(
        keep,
        in_specs=[whole()] * 4,
        out_specs=whole(),
        out_shape=pltpu.VMEM((rows, LATENT + LANES), jnp.int16),
        scratch_shapes=[pltpu.VMEM((rows, LATENT), F32)] * 2,
        compiler_params=pltpu.CompilerParams(vmem_limit_bytes=16 * 2**20),
        cost_estimate=cost(LATENT),
        name="keep",
    )(score, peaks, keys, lent)
    packed = packed.reshape(chips, rows // chips, LATENT + LANES)
    packed = lax.all_to_all(packed, CHIPS, 0, 0, tiled=True)
    copies = pl.pallas_call(
        finish,
        in_specs=[whole()],
        out_specs=whole(),
        out_shape=pltpu.VMEM((chips, rows // chips, LATENT), jnp.bfloat16),
        compiler_params=pltpu.CompilerParams(vmem_limit_bytes=8 * 2**20),
        name="finish",
    )(packed)
    mine = lax.all_to_all(copies, CHIPS, 0, 0, tiled=True).reshape(rows, LATENT)
    other = lax.ppermute(mine, CORE, swap)
    both = pl.pallas_call(
        place_own,
        in_specs=[whole()],
        out_specs=anywhere(),
        out_shape=out,
        scratch_shapes=[pltpu.SemaphoreType.DMA(())],
        compiler_params=pltpu.CompilerParams(vmem_limit_bytes=2**20),
        cost_estimate=pl.CostEstimate(flops=10**7, bytes_accessed=4 * rows * LATENT, transcendentals=0),
        name="place_own",
    )(mine)
    both = pl.pallas_call(
        place_other,
        in_specs=[whole(), anywhere()],
        out_specs=anywhere(),
        out_shape=out,
        input_output_aliases={1: 0},
        scratch_shapes=[pltpu.SemaphoreType.DMA(())],
        compiler_params=pltpu.CompilerParams(vmem_limit_bytes=2**20),
        name="place_other",
    )(other, both)
    return both.reshape(requests, qtokens, heads, LATENT)


def solution(mesh):
    torus = Mesh(mesh.devices.reshape(4, 4, 4, 2), SEQ)
    in_specs = (P(), P(None, SEQ, None), P(), P())
    return jax.shard_map(
        on_device, mesh=torus, in_specs=in_specs, out_specs=P(), check_vma=False
    )
```
